32 devices in a mesh: dp: 1 (over z), yax: 4 (over y), xax: 8 (over x, core).
Axes of the slice: x: 4, y: 4, z: 1, core: 2. Of those that a mesh axis runs over, the one named last changes fastest.
The devices are a block of a 4x4x8 slice.
Arguments:
- hidden: bfloat16 [384, 2560], P('dp', 'xax')
- cache_len: int32 [384], P('dp')
- k_cache: bfloat16 [384, 8192, 80], P(('dp', 'yax', 'xax'))
- v_cache: bfloat16 [384, 8192, 80], P(('dp', 'yax', 'xax'))
- g_attn: float32 [2560], P('xax')
- w_query: bfloat16 [2560, 2560], P('xax', 'yax')
- w_key: bfloat16 [2560, 80], P('xax')
- w_value: bfloat16 [2560, 80], P('xax')
- w_gate: bfloat16 [2560, 10240], P('xax', 'yax')
- w_up: bfloat16 [2560, 10240], P('xax', 'yax')
- w_out: bfloat16 [2560, 2560], P('yax', 'xax')
- w_down: bfloat16 [10240, 2560], P('yax', 'xax')
- g_final: float32 [2560], P('xax')
- embedding: bfloat16 [50304, 2560], P('yax', 'xax')
Outputs:
- output 1: bfloat16 [384, 80], P(('dp', 'yax', 'xax'))
- output 2: bfloat16 [384, 80], P(('dp', 'yax', 'xax'))
- output 3: float32 [384, 50304], P('dp', ('yax', 'xax'))
- output 4: float32 [384], P('dp')
All inputs are finite; a program needn't handle non-finite values.
Results may differ from the reference program's by a relative error of at most 0.00114.
Values are sent between devices in bfloat16 or wider.
A program may use at most 768 MiB of HBM per device.

```python
import jax
import jax.numpy as jnp
from jax import lax

D = 2560
HEADS = 32
HEAD = 80
FF = 10240
VOCAB = 50304
BATCH = 384
SEQ = 8192
ROW_BLOCK = 16

EPS = 1e-6
ROPE_BASE = 10000.0


def draw_lengths(key):
    drawn = jax.random.randint(key, (BATCH,), 1, SEQ, dtype=jnp.int32)
    row_ids = jnp.arange(BATCH)
    return jnp.where(row_ids == 0, SEQ - 1, jnp.where(row_ids == 1, 1, drawn)).astype(jnp.int32)


def setup_inputs(seed: int = 0, part: int = 0) -> dict:
    base_key = jax.random.key(seed)
    shared = jax.random.split(base_key, 10)
    own = jax.random.split(jax.random.fold_in(base_key, part), 5)

    def weight(key, shape, fan_in, gain):
        return (gain * fan_in ** -0.5 * jax.random.normal(key, shape, jnp.float32)).astype(jnp.bfloat16)

    col_scale = jnp.exp(0.5 * jax.random.normal(own[0], (D,), jnp.float32))
    hidden = jax.random.normal(own[1], (BATCH, D), jnp.float32) * col_scale
    k_cache = 2.5 * jax.random.normal(own[3], (BATCH, SEQ, HEAD), jnp.float32)
    v_cache = 2.0 * jax.random.normal(own[4], (BATCH, SEQ, HEAD), jnp.float32)
    return {
        "hidden": hidden.astype(jnp.bfloat16),
        "cache_len": draw_lengths(own[2]),
        "k_cache": k_cache.astype(jnp.bfloat16),
        "v_cache": v_cache.astype(jnp.bfloat16),
        "g_attn": 1.0 + 0.3 * jax.random.normal(shared[0], (D,), jnp.float32),
        "w_query": weight(shared[1], (D, HEADS * HEAD), D, 1.0),
        "w_key": weight(shared[2], (D, HEAD), D, 1.0),
        "w_value": weight(shared[3], (D, HEAD), D, 1.0),
        "w_gate": weight(shared[4], (D, FF), D, 1.0),
        "w_up": weight(shared[5], (D, FF), D, 1.0),
        "w_out": weight(shared[6], (HEADS * HEAD, D), HEADS * HEAD, 1.0),
        "w_down": weight(shared[7], (FF, D), FF, 1.0),
        "g_final": 1.0 + 0.3 * jax.random.normal(shared[8], (D,), jnp.float32),
        "embedding": weight(shared[9], (VOCAB, D), D, 2.0),
    }


def layer_norm(values_in, gain):
    row_mean = jnp.mean(values_in, axis=-1, keepdims=True)
    row_var = jnp.mean(jnp.square(values_in - row_mean), axis=-1, keepdims=True)
    return (values_in - row_mean) * lax.rsqrt(row_var + EPS) * gain


def rope_angle(positions):
    half_dim = HEAD // 2
    inv_freq = ROPE_BASE ** (-(jnp.arange(half_dim, dtype=jnp.float32) * 2.0) / HEAD)
    return positions.astype(jnp.float32)[:, None] * inv_freq[None, :]


def rotary(values_in, angles):
    half_dim = values_in.shape[-1] // 2
    cos_a = jnp.cos(angles)
    sin_a = jnp.sin(angles)
    first = values_in[..., :half_dim]
    second = values_in[..., half_dim:]
    return jnp.concatenate([first * cos_a - second * sin_a, second * cos_a + first * sin_a], axis=-1)


def attend_block(block):
    q_blk, kc_blk, vc_blk, kn_blk, vn_blk, len_blk = block
    positions = jnp.arange(SEQ)
    at_slot = positions[None, :, None] == len_blk[:, None, None]
    keys_all = jnp.where(at_slot, kn_blk[:, None, :], kc_blk)
    values_all = jnp.where(at_slot, vn_blk[:, None, :], vc_blk)
    scores = jnp.einsum("rhe,rse->rhs", q_blk.astype(jnp.float32), keys_all.astype(jnp.float32)) * HEAD ** -0.5
    valid = positions[None, None, :] <= len_blk[:, None, None]
    scores = jnp.where(valid, scores, -jnp.inf)
    prob_all = jax.nn.softmax(scores, axis=-1).astype(jnp.bfloat16)
    mixed = jnp.einsum("rhs,rse->rhe", prob_all.astype(jnp.float32), values_all.astype(jnp.float32))
    return mixed.astype(jnp.bfloat16)


def reference(hidden, cache_len, k_cache, v_cache, g_attn, w_query, w_key, w_value,
              w_gate, w_up, w_out, w_down, g_final, embedding):
    residual = hidden.astype(jnp.float32)
    normed = layer_norm(residual, g_attn).astype(jnp.bfloat16)
    query = jnp.dot(normed, w_query, preferred_element_type=jnp.float32).astype(jnp.bfloat16)
    key_new = jnp.dot(normed, w_key, preferred_element_type=jnp.float32).astype(jnp.bfloat16)
    value_new = jnp.dot(normed, w_value, preferred_element_type=jnp.float32).astype(jnp.bfloat16)
    gate = jnp.dot(normed, w_gate, preferred_element_type=jnp.float32).astype(jnp.bfloat16)
    up_val = jnp.dot(normed, w_up, preferred_element_type=jnp.float32).astype(jnp.bfloat16)
    angles = rope_angle(cache_len)
    query = rotary(query.astype(jnp.float32).reshape(BATCH, HEADS, HEAD), angles[:, None, :]).astype(jnp.bfloat16)
    key_new = rotary(key_new.astype(jnp.float32), angles).astype(jnp.bfloat16)
    blocks = BATCH // ROW_BLOCK
    attn_out = lax.map(attend_block, (
        query.reshape(blocks, ROW_BLOCK, HEADS, HEAD),
        k_cache.reshape(blocks, ROW_BLOCK, SEQ, HEAD),
        v_cache.reshape(blocks, ROW_BLOCK, SEQ, HEAD),
        key_new.reshape(blocks, ROW_BLOCK, HEAD),
        value_new.reshape(blocks, ROW_BLOCK, HEAD),
        cache_len.reshape(blocks, ROW_BLOCK)))
    attn_out = attn_out.reshape(BATCH, HEADS * HEAD)
    mlp_act = (jax.nn.silu(gate.astype(jnp.float32)) * up_val.astype(jnp.float32)).astype(jnp.bfloat16)
    branch_sum = (jnp.dot(attn_out, w_out, preferred_element_type=jnp.float32)
                  + jnp.dot(mlp_act, w_down, preferred_element_type=jnp.float32))
    residual_out = residual + branch_sum
    final_norm = layer_norm(residual_out, g_final).astype(jnp.bfloat16)
    logits = jnp.dot(final_norm, embedding.T, preferred_element_type=jnp.float32)
    log_norm = jax.nn.logsumexp(logits, axis=-1)
    return key_new, value_new, logits - log_norm[:, None], log_norm
```

```python
import functools
import itertools

import jax
import jax.numpy as jnp
from jax import lax
from jax.experimental import pallas as pl
from jax.experimental.pallas import tpu as pltpu
from jax.sharding import PartitionSpec as P

EPS = 1e-6
ROPE_BASE = 10000.0
LANES = 128
CORES = 2


def rope_angle(positions, head_dim):
    half_dim = head_dim // 2
    inv_freq = ROPE_BASE ** (-(jnp.arange(half_dim, dtype=jnp.float32) * 2.0) / head_dim)
    return positions.astype(jnp.float32)[:, None] * inv_freq[None, :]


def rotary(values_in, angles):
    half_dim = values_in.shape[-1] // 2
    cos_a = jnp.cos(angles)
    sin_a = jnp.sin(angles)
    first = values_in[..., :half_dim]
    second = values_in[..., half_dim:]
    return jnp.concatenate([first * cos_a - second * sin_a, second * cos_a + first * sin_a], axis=-1)


def attend_local(query, k_cache, v_cache, key_new, value_new, lengths):
    score_scale = query.shape[-1] ** -0.5
    scores = jnp.einsum("bhe,bse->bhs", query, k_cache, preferred_element_type=jnp.float32) * score_scale
    score_new = jnp.einsum("bhe,be->bh", query, key_new, preferred_element_type=jnp.float32) * score_scale
    valid = jnp.arange(k_cache.shape[1])[None, None, :] < lengths[:, None, None]
    row_max = jnp.maximum(jnp.max(jnp.where(valid, scores, -jnp.inf), axis=-1), score_new)
    weights = jnp.where(valid, jnp.exp(scores - row_max[..., None]), 0.0)
    weight_new = jnp.exp(score_new - row_max)
    denominator = jnp.sum(weights, axis=-1) + weight_new
    prob_all = (weights / denominator[..., None]).astype(jnp.bfloat16)
    prob_new = (weight_new / denominator).astype(jnp.bfloat16)
    attn_out = jnp.einsum("bhs,bse->bhe", prob_all, v_cache, preferred_element_type=jnp.float32)
    attn_out = attn_out + prob_new.astype(jnp.float32)[..., None] * value_new.astype(jnp.float32)[:, None, :]
    return attn_out.astype(jnp.bfloat16)


def my_coords():
    x_idx = lax.axis_index("xax")
    return {"y": lax.axis_index("yax"), "X": lax.div(x_idx, CORES), "c": lax.rem(x_idx, CORES)}


def flat_index(coords, axes, sizes):
    index = 0
    for axis in axes:
        index = index * sizes[axis] + coords[axis]
    return index


def exchange(items, sizes, collective_id):
    plan = []
    for array, group, by in items:
        offsets = list(itertools.product(*[range(sizes[a]) for a in group]))[1:]
        block = array.shape[1:] if by else array.shape
        plan.append((group, by, offsets, block, array.dtype))
    peer_offsets = sorted({tuple(dict(zip(group, off)).get(a, 0) for a in ("y", "X", "c"))
                           for group, _, offsets, _, _ in plan for off in offsets})
    n_items = len(items)
    most = max(len(p[2]) for p in plan)

    def target(me, off):
        coords = {a: lax.rem(me[a] + off.get(a, 0), sizes[a]) for a in me}
        return coords, {"yax": coords["y"], "xax": coords["X"] * CORES + coords["c"]}

    def kernel(*refs):
        ins, outs = refs[:n_items], refs[n_items:2 * n_items]
        send_sem, recv_sem = refs[2 * n_items:]
        me = my_coords()
        barrier = pltpu.get_barrier_semaphore()
        for off in peer_offsets:
            _, device = target(me, dict(zip(("y", "X", "c"), off)))
            pl.semaphore_signal(barrier, inc=1, device_id=device, device_id_type=pl.DeviceIdType.MESH)
        pl.semaphore_wait(barrier, len(peer_offsets))
        copies = []
        for i, (group, by, offsets, _, _) in enumerate(plan):
            slot = flat_index(me, group, sizes)
            for j, off in enumerate(offsets):
                coords, device = target(me, dict(zip(group, off)))
                src = ins[i].at[flat_index(coords, by, sizes)] if by else ins[i]
                copy = pltpu.make_async_remote_copy(
                    src_ref=src, dst_ref=outs[i].at[slot], send_sem=send_sem.at[i, j], recv_sem=recv_sem.at[i, j],
                    device_id=device, device_id_type=pl.DeviceIdType.MESH)
                copy.start()
                copies.append(copy)
            outs[i][slot] = ins[i][flat_index(me, by, sizes)] if by else ins[i][...]
        for copy in copies:
            copy.wait()

    out = pl.pallas_call(
        kernel,
        out_shape=[jax.ShapeDtypeStruct((len(offsets) + 1,) + tuple(block), dtype)
                   for _, _, offsets, block, dtype in plan],
        in_specs=[pl.BlockSpec(memory_space=pltpu.VMEM)] * n_items,
        out_specs=[pl.BlockSpec(memory_space=pltpu.VMEM)] * n_items,
        scratch_shapes=[pltpu.SemaphoreType.DMA((n_items, most)), pltpu.SemaphoreType.DMA((n_items, most))],
        compiler_params=pltpu.CompilerParams(collective_id=collective_id, has_side_effects=True),
        name=f"exchange{collective_id}",
    )(*[item[0] for item in items])
    return out


def split_vocab(emb_t, tail, own, n_parts, width):
    depth, vocab = emb_t.shape
    part = vocab // n_parts
    window = width + LANES
    whole = vocab // LANES * LANES

    def kernel(emb_ref, tail_ref, out_ref, raw, cut, in_sem, tail_sem, out_sem):
        x_idx = lax.axis_index("xax")
        loads = []
        for k in range(n_parts):
            start = part * k // LANES * LANES
            size = min(window, whole - start)
            ops = [pltpu.make_async_copy(emb_ref.at[:, pl.ds(start, size)], raw.at[k, :, pl.ds(0, size)], in_sem.at[k])]
            if size < window:
                ops.append(pltpu.make_async_copy(tail_ref, raw.at[k, :, pl.ds(size, LANES)], tail_sem))
            for op in ops:
                op.start()
            loads.append(ops)
        stores = []
        for k in range(n_parts):
            for op in loads[k]:
                op.wait()
            shift = part * k % LANES
            cut[k] = raw[k, :, shift:shift + width]
            op = pltpu.make_async_copy(cut.at[k], out_ref.at[lax.rem(k - x_idx + n_parts, n_parts)], out_sem.at[k])
            op.start()
            stores.append(op)
        for op in stores:
            op.wait()

    return pl.pallas_call(
        kernel,
        out_shape=jax.ShapeDtypeStruct((n_parts, depth, width), emb_t.dtype),
        in_specs=[pl.BlockSpec(memory_space=pl.ANY), pl.BlockSpec(memory_space=pl.ANY)],
        out_specs=pl.BlockSpec(memory_space=pl.ANY),
        scratch_shapes=[pltpu.VMEM((n_parts, depth, window), emb_t.dtype), pltpu.VMEM((n_parts, depth, width), emb_t.dtype),
                        pltpu.SemaphoreType.DMA((n_parts,)), pltpu.SemaphoreType.DMA, pltpu.SemaphoreType.DMA((n_parts,))],
        compiler_params=pltpu.CompilerParams(vmem_limit_bytes=40 << 20),
        name="split_vocab",
    )(emb_t, tail)


def after(value, *others):
    return lax.optimization_barrier((value,) + others)[0]


def solution(mesh):
    y_size = mesh.shape["yax"]
    x_size = mesh.shape["xax"]
    chips = x_size // CORES
    sizes = {"y": y_size, "X": chips, "c": CORES}
    row_spec = P(("dp", "yax", "xax"))

    def shift(value, step):
        return lax.ppermute(value, "xax", [(i, (i + step) % x_size) for i in range(x_size)])

    def contract(lhs, rhs, dims):
        return lax.dot_general(lhs, rhs, (dims, ((), ())), preferred_element_type=jnp.float32)

    def local_step(hidden, cache_len, k_cache, v_cache, g_attn, w_query, w_key, w_value,
                   w_gate, w_up, w_out, w_down, g_final, embedding):
        rows = hidden.shape[0]
        depth = hidden.shape[1]
        width = depth * x_size
        own_rows = k_cache.shape[0]
        head_dim = k_cache.shape[2]
        q_cols = w_query.shape[1]
        heads = q_cols // head_dim
        ff = w_gate.shape[1]
        ff_chip = ff // chips
        vocab = embedding.shape[0]
        own_vocab = vocab // x_size
        me = my_coords()
        y_idx, x_idx, chip, core = me["y"], lax.axis_index("xax"), me["X"], me["c"]
        own_start = (y_idx * x_size + x_idx) * own_rows

        gate_up = jnp.stack([jnp.stack([w_gate[:, ff_chip * i:ff_chip * (i + 1)], w_up[:, ff_chip * i:ff_chip * (i + 1)]])
                             for i in range(chips)])
        gu_parts = []
        for s in range(chips):
            part = lax.dynamic_index_in_dim(gate_up, lax.rem(chip + s, chips), 0, keepdims=False)
            gu_parts.append(part if s == 0 else shift(part, CORES * s))

        hid_t = hidden.T
        res_t = hid_t.astype(jnp.float32)
        stats = jnp.stack([jnp.sum(res_t, axis=0), jnp.sum(res_t * res_t, axis=0)])
        (stats,) = exchange([(stats, ("X", "c"), ())], sizes, 1)
        stats = jnp.sum(stats, axis=0)
        mean = stats[0] / width
        var = stats[1] / width - mean * mean
        norm_t = ((res_t - mean[None]) * lax.rsqrt(var + EPS)[None] * g_attn[:, None]).astype(jnp.bfloat16)

        q_part = contract(norm_t, w_query, ((0,), (0,))).reshape(y_size * x_size, own_rows, q_cols)
        kv_part = contract(norm_t, jnp.concatenate([w_key, w_value], axis=1), ((0,), (0,)))
        kv_part = lax.dynamic_slice_in_dim(kv_part, y_idx * x_size * own_rows, x_size * own_rows, axis=0)
        kv_part = kv_part.reshape(x_size, own_rows, 2 * head_dim)
        q_all, kv_all, norm_all = exchange(
            [(q_part, ("y", "X", "c"), ("y", "X", "c")), (kv_part, ("X", "c"), ("X", "c")),
             (norm_t, ("X",), ())], sizes, 2)
        len_own = lax.dynamic_slice_in_dim(cache_len, own_start, own_rows, axis=0)
        angles = rope_angle(len_own, head_dim)
        query = jnp.sum(q_all.reshape(y_size, x_size, own_rows, q_cols), axis=1).astype(jnp.bfloat16)
        query = query.reshape(y_size, own_rows, heads, head_dim).transpose(1, 0, 2, 3)
        query = query.reshape(own_rows, y_size * heads, head_dim)
        query_own = rotary(query.astype(jnp.float32), angles[:, None, :]).astype(jnp.bfloat16)
        kv_own = jnp.sum(kv_all, axis=0).astype(jnp.bfloat16)
        key_own = rotary(kv_own[:, :head_dim].astype(jnp.float32), angles).astype(jnp.bfloat16)
        value_own = kv_own[:, head_dim:]

        padded = -(-own_vocab // LANES) * LANES
        whole = vocab // LANES * LANES
        emb_t = embedding.T
        tail = jnp.pad(emb_t[:, whole:], ((0, 0), (0, LANES - (vocab - whole))))
        emb_parts = split_vocab(after(emb_t, q_all), tail, x_idx, x_size, padded)
        emb_got = {0: emb_parts[0]}
        for s in (2, 6):
            emb_got[s] = shift(emb_parts[s], s)

        attn_own = attend_local(query_own, k_cache, v_cache, key_own, value_own, len_own)
        attn_blocks = attn_own.reshape(own_rows, y_size, q_cols).transpose(1, 0, 2)

        gu_sum = 0.0
        for s in range(chips):
            block = lax.dynamic_index_in_dim(norm_all, lax.rem(chip - s + chips, chips), 0, keepdims=False)
            gu_sum = gu_sum + contract(gu_parts[s].transpose(1, 0, 2).reshape(depth, 2 * ff_chip), block, ((0,), (0,)))
        half = ff_chip // CORES
        gu_sum = gu_sum.reshape(2, CORES, half, rows).transpose(1, 0, 2, 3)
        (gu_sum,) = exchange([(gu_sum, ("c",), ("c",))], sizes, 3)
        gu_sum = jnp.sum(gu_sum, axis=0).astype(jnp.bfloat16)
        mlp_t = (jax.nn.silu(gu_sum[0].astype(jnp.float32)) * gu_sum[1].astype(jnp.float32)).astype(jnp.bfloat16)
        attn_all, mlp_all = exchange([(attn_blocks, ("y", "X", "c"), ("y",)), (mlp_t, ("X",), ())], sizes, 4)
        (mlp_all,) = exchange([(mlp_all, ("c",), ())], sizes, 5)
        for s in (3, 5, 1):
            emb_got[s] = shift(after(emb_parts[s], mlp_all), s)
        mlp_all = mlp_all.transpose(1, 0, 2, 3).reshape(ff, rows)
        branch = (contract(w_out.T, attn_all.reshape(rows, q_cols), ((1,), (1,)))
                  + contract(w_down.T, mlp_all, ((1,), (0,))))

        sub = depth // y_size
        (branch,) = exchange([(branch.reshape(y_size, sub, rows), ("y",), ("y",))], sizes, 6)
        r_t = lax.dynamic_slice_in_dim(res_t, y_idx * sub, sub, axis=0) + jnp.sum(branch, axis=0)
        stats = jnp.stack([jnp.sum(r_t, axis=0), jnp.sum(r_t * r_t, axis=0)])
        (stats,) = exchange([(stats, ("y", "X", "c"), ())], sizes, 7)
        stats = jnp.sum(stats, axis=0)
        mean = stats[0] / width
        var = stats[1] / width - mean * mean
        gain = lax.dynamic_slice_in_dim(g_final, y_idx * sub, sub, axis=0)
        f_t = ((r_t - mean[None]) * lax.rsqrt(var + EPS)[None] * gain[:, None]).astype(jnp.bfloat16)
        (f_t,) = exchange([(f_t, ("X",), ())], sizes, 8)
        for s in (4, 7):
            emb_got[s] = shift(after(emb_parts[s], f_t), s)
        (f_t,) = exchange([(f_t, ("y",), ())], sizes, 9)
        (f_t,) = exchange([(f_t, ("c",), ())], sizes, 10)
        f_t = f_t.transpose(2, 0, 1, 3, 4).reshape(x_size, depth, rows)

        logits = 0.0
        for s in (0, 2, 6, 1, 3, 5, 4, 7):
            block = lax.dynamic_index_in_dim(f_t, lax.rem(x_idx - s + x_size, x_size), 0, keepdims=False)
            logits = logits + contract(emb_got[s], block, ((0,), (0,)))
        logits = logits[:own_vocab]
        row_max = jnp.max(logits, axis=0)
        sum_exp = jnp.sum(jnp.exp(logits - row_max[None]), axis=0)
        (shares,) = exchange([(jnp.stack([row_max, sum_exp]), ("y", "X", "c"), ())], sizes, 11)
        top = jnp.max(shares[:, 0], axis=0)
        log_norm = top + jnp.log(jnp.sum(shares[:, 1] * jnp.exp(shares[:, 0] - top[None]), axis=0))
        return key_own, value_own, (logits - log_norm[None]).T, log_norm

    in_specs = (P("dp", "xax"), P("dp"), row_spec, row_spec, P("xax"), P("xax", "yax"),
                P("xax", None), P("xax", None), P("xax", "yax"), P("xax", "yax"),
                P("yax", "xax"), P("yax", "xax"), P("xax"), P("yax", "xax"))
    out_specs = (row_spec, row_spec, P("dp", ("yax", "xax")), P("dp"))
    return jax.shard_map(local_step, mesh=mesh, in_specs=in_specs, out_specs=out_specs, check_vma=False)
```

```python
import functools
import itertools

import jax
import jax.numpy as jnp
from jax import lax
from jax.experimental import pallas as pl
from jax.experimental.pallas import tpu as pltpu
from jax.sharding import PartitionSpec as P

EPS = 1e-6
ROPE_BASE = 10000.0
LANES = 128
CORES = 2


def rope_angle(positions, head_dim):
    half_dim = head_dim // 2
    inv_freq = ROPE_BASE ** (-(jnp.arange(half_dim, dtype=jnp.float32) * 2.0) / head_dim)
    return positions.astype(jnp.float32)[:, None] * inv_freq[None, :]


def rotary(values_in, angles):
    half_dim = values_in.shape[-1] // 2
    cos_a = jnp.cos(angles)
    sin_a = jnp.sin(angles)
    first = values_in[..., :half_dim]
    second = values_in[..., half_dim:]
    return jnp.concatenate([first * cos_a - second * sin_a, second * cos_a + first * sin_a], axis=-1)


def attend_local(query, k_cache, v_cache, key_new, value_new, lengths):
    score_scale = query.shape[-1] ** -0.5
    scores = jnp.einsum("bhe,bse->bhs", query, k_cache, preferred_element_type=jnp.float32) * score_scale
    score_new = jnp.einsum("bhe,be->bh", query, key_new, preferred_element_type=jnp.float32) * score_scale
    valid = jnp.arange(k_cache.shape[1])[None, None, :] < lengths[:, None, None]
    row_max = jnp.maximum(jnp.max(jnp.where(valid, scores, -jnp.inf), axis=-1), score_new)
    weights = jnp.where(valid, jnp.exp(scores - row_max[..., None]), 0.0)
    weight_new = jnp.exp(score_new - row_max)
    denominator = jnp.sum(weights, axis=-1) + weight_new
    prob_all = (weights / denominator[..., None]).astype(jnp.bfloat16)
    prob_new = (weight_new / denominator).astype(jnp.bfloat16)
    attn_out = jnp.einsum("bhs,bse->bhe", prob_all, v_cache, preferred_element_type=jnp.float32)
    attn_out = attn_out + prob_new.astype(jnp.float32)[..., None] * value_new.astype(jnp.float32)[:, None, :]
    return attn_out.astype(jnp.bfloat16)


def my_coords():
    x_idx = lax.axis_index("xax")
    return {"y": lax.axis_index("yax"), "X": lax.div(x_idx, CORES), "c": lax.rem(x_idx, CORES)}


def flat_index(coords, axes, sizes):
    index = 0
    for axis in axes:
        index = index * sizes[axis] + coords[axis]
    return index


def exchange(items, sizes, collective_id):
    plan = []
    for array, group, by in items:
        offsets = list(itertools.product(*[range(sizes[a]) for a in group]))[1:]
        block = array.shape[1:] if by else array.shape
        plan.append((group, by, offsets, block, array.dtype))
    peer_offsets = sorted({tuple(dict(zip(group, off)).get(a, 0) for a in ("y", "X", "c"))
                           for group, _, offsets, _, _ in plan for off in offsets})
    n_items = len(items)
    most = max(len(p[2]) for p in plan)

    def target(me, off):
        coords = {a: lax.rem(me[a] + off.get(a, 0), sizes[a]) for a in me}
        return coords, {"yax": coords["y"], "xax": coords["X"] * CORES + coords["c"]}

    def kernel(*refs):
        ins, outs = refs[:n_items], refs[n_items:2 * n_items]
        send_sem, recv_sem = refs[2 * n_items:]
        me = my_coords()
        barrier = pltpu.get_barrier_semaphore()
        for off in peer_offsets:
            _, device = target(me, dict(zip(("y", "X", "c"), off)))
            pl.semaphore_signal(barrier, inc=1, device_id=device, device_id_type=pl.DeviceIdType.MESH)
        pl.semaphore_wait(barrier, len(peer_offsets))
        copies = []
        for i, (group, by, offsets, _, _) in enumerate(plan):
            slot = flat_index(me, group, sizes)
            for j, off in enumerate(offsets):
                coords, device = target(me, dict(zip(group, off)))
                src = ins[i].at[flat_index(coords, by, sizes)] if by else ins[i]
                copy = pltpu.make_async_remote_copy(
                    src_ref=src, dst_ref=outs[i].at[slot], send_sem=send_sem.at[i, j], recv_sem=recv_sem.at[i, j],
                    device_id=device, device_id_type=pl.DeviceIdType.MESH)
                copy.start()
                copies.append(copy)
            outs[i][slot] = ins[i][flat_index(me, by, sizes)] if by else ins[i][...]
        for copy in copies:
            copy.wait()

    out = pl.pallas_call(
        kernel,
        out_shape=[jax.ShapeDtypeStruct((len(offsets) + 1,) + tuple(block), dtype)
                   for _, _, offsets, block, dtype in plan],
        in_specs=[pl.BlockSpec(memory_space=pltpu.VMEM)] * n_items,
        out_specs=[pl.BlockSpec(memory_space=pltpu.VMEM)] * n_items,
        scratch_shapes=[pltpu.SemaphoreType.DMA((n_items, most)), pltpu.SemaphoreType.DMA((n_items, most))],
        compiler_params=pltpu.CompilerParams(collective_id=collective_id, has_side_effects=True),
        name=f"exchange{collective_id}",
    )(*[item[0] for item in items])
    return out


def split_vocab(emb_t, tail, n_parts, width):
    depth, vocab = emb_t.shape
    part = vocab // n_parts
    window = width + LANES
    whole = vocab // LANES * LANES

    def kernel(emb_ref, tail_ref, out_ref, raw, cut, in_sem, tail_sem, out_sem):
        me = my_coords()
        chips = n_parts // CORES
        loads = []
        for k in range(n_parts):
            start = part * k // LANES * LANES
            size = min(window, whole - start)
            ops = [pltpu.make_async_copy(emb_ref.at[:, pl.ds(start, size)], raw.at[k, :, pl.ds(0, size)], in_sem.at[k])]
            if size < window:
                ops.append(pltpu.make_async_copy(tail_ref, raw.at[k, :, pl.ds(size, LANES)], tail_sem))
            for op in ops:
                op.start()
            loads.append(ops)
        stores = []
        for k in range(n_parts):
            for op in loads[k]:
                op.wait()
            shift = part * k % LANES
            cut[k] = raw[k, :, shift:shift + width]
            slot = lax.rem(k // CORES - me["X"] + chips, chips) * CORES + lax.rem(k % CORES + me["c"], CORES)
            op = pltpu.make_async_copy(cut.at[k], out_ref.at[slot], out_sem.at[k])
            op.start()
            stores.append(op)
        for op in stores:
            op.wait()

    return pl.pallas_call(
        kernel,
        out_shape=jax.ShapeDtypeStruct((n_parts, depth, width), emb_t.dtype),
        in_specs=[pl.BlockSpec(memory_space=pl.ANY), pl.BlockSpec(memory_space=pl.ANY)],
        out_specs=pl.BlockSpec(memory_space=pl.ANY),
        scratch_shapes=[pltpu.VMEM((n_parts, depth, window), emb_t.dtype), pltpu.VMEM((n_parts, depth, width), emb_t.dtype),
                        pltpu.SemaphoreType.DMA((n_parts,)), pltpu.SemaphoreType.DMA, pltpu.SemaphoreType.DMA((n_parts,))],
        compiler_params=pltpu.CompilerParams(vmem_limit_bytes=40 << 20),
        name="split_vocab",
    )(emb_t, tail)


def pick_columns(arrays, chip, chips):
    depth, columns = arrays[0].shape
    block = columns // chips
    n = len(arrays)

    def kernel(*refs):
        ins, outs, sem = refs[:n], refs[n:n + chips], refs[n + chips]
        chip_idx = lax.div(lax.axis_index("xax"), CORES)
        copies = []
        for s in range(chips):
            start = pl.multiple_of(lax.rem(chip_idx + s, chips) * block, LANES)
            for i in range(n):
                copy = pltpu.make_async_copy(ins[i].at[:, pl.ds(start, block)], outs[s].at[i], sem.at[s, i])
                copy.start()
                copies.append(copy)
        for copy in copies:
            copy.wait()

    return pl.pallas_call(
        kernel,
        out_shape=[jax.ShapeDtypeStruct((n, depth, block), arrays[0].dtype)] * chips,
        in_specs=[pl.BlockSpec(memory_space=pl.ANY)] * n,
        out_specs=[pl.BlockSpec(memory_space=pltpu.VMEM)] * chips,
        scratch_shapes=[pltpu.SemaphoreType.DMA((chips, n))],
        name="pick_columns",
    )(*arrays)


def mix_and_norm(gate_up, attn_blocks, res_sub, gain_sub, w_out_t, w_down_t, sizes, width, collective_id):
    n_y, n_chip = sizes["y"], sizes["X"]
    n_x = n_chip * CORES
    n_all = n_y * n_x
    half, rows = gate_up.shape[2:]
    depth = w_out_t.shape[0]
    sub = depth // n_y
    seqs, q_cols = attn_blocks.shape[1:]
    own_rows = rows // n_all
    offsets = list(itertools.product(range(n_y), range(n_chip), range(CORES)))[1:]
    far = [s for s in (1, n_chip - 1) + tuple(range(2, n_chip - 1)) if s]

    def kernel(gu_ref, attn_ref, res_ref, gain_ref, wo_ref, wd_ref, f_ref, gu_got, m_all, o_all, br, rs, st,
               core_sem, m_sem, md_sem, o_sem, rs_sem, st_sem, fx_sem, fy_sem, fd_sem):
        me = my_coords()
        y, chip, core = me["y"], me["X"], me["c"]
        x = chip * CORES + core
        index = y * n_x + x

        def device(dy=0, dchip=0, dcore=0):
            return {"yax": lax.rem(y + dy, n_y),
                    "xax": lax.rem(chip + dchip, n_chip) * CORES + lax.rem(core + dcore, CORES)}

        def start(src, dst, sems, at, **to):
            copy = pltpu.make_async_remote_copy(src_ref=src, dst_ref=dst, send_sem=sems.at[(0,) + at],
                                                recv_sem=sems.at[(1,) + at], device_id=device(**to),
                                                device_id_type=pl.DeviceIdType.MESH)
            copy.start()
            return copy

        barrier = pltpu.get_barrier_semaphore()
        for dy, dchip, dcore in offsets:
            pl.semaphore_signal(barrier, inc=1, device_id=device(dy, dchip, dcore), device_id_type=pl.DeviceIdType.MESH)
        pl.semaphore_wait(barrier, len(offsets))

        sent = []
        gu_copy = start(gu_ref.at[1 - core], gu_got, core_sem, (), dcore=1)
        sent.append(gu_copy)

        gu_copy.wait_recv()
        total = (gu_ref[core] + gu_got[...]).astype(jnp.bfloat16).astype(jnp.float32)
        m_own = m_all.at[pl.ds(pl.multiple_of(x * half, half), half)]
        m_own[...] = (jax.nn.silu(total[0]) * total[1]).astype(jnp.bfloat16)
        m_copies = {s: start(m_own, m_own, m_sem, (s,), dchip=s) for s in far}
        o_own = o_all.at[pl.ds(pl.multiple_of(index * seqs, seqs), seqs)]
        o_copies = []
        for j, (dy, dchip, dcore) in enumerate(offsets):
            o_copies.append(start(attn_ref.at[lax.rem(y + dy, n_y)], o_own, o_sem, (j,), dy=dy, dchip=dchip, dcore=dcore))
        md_copies = [start(m_own, m_own, md_sem, (0,), dcore=1)]
        o_own[...] = attn_ref[y]
        for s in far:
            m_copies[s].wait_recv()
            source = lax.rem(chip - s + n_chip, n_chip) * CORES + core
            block = m_all.at[pl.ds(pl.multiple_of(source * half, half), half)]
            md_copies.append(start(block, block, md_sem, (s,), dcore=1))
        for copy in o_copies:
            copy.wait_recv()
        row = lax.broadcasted_iota(jnp.int32, (n_all * seqs, rows), 0)
        col = lax.broadcasted_iota(jnp.int32, (n_all * seqs, rows), 1)
        seq = row // seqs * own_rows + row % seqs
        pick = jnp.where((seq == col) & (row % seqs < own_rows), 1.0, 0.0).astype(jnp.bfloat16)
        heads = lax.dot_general(o_all[...], pick, (((0,), (0,)), ((), ())),
                                preferred_element_type=jnp.float32).astype(jnp.bfloat16)
        branch = jnp.dot(wo_ref[...], heads, preferred_element_type=jnp.float32)
        for copy in md_copies:
            copy.wait_recv()
        br[...] = branch + jnp.dot(wd_ref[...], m_all[...], preferred_element_type=jnp.float32)

        rs_copies = []
        for dy in range(1, n_y):
            part = br.at[pl.ds(pl.multiple_of(lax.rem(y + dy, n_y) * sub, sub), sub)]
            rs_copies.append(start(part, rs.at[y], rs_sem, (dy,), dy=dy))
        rs[y] = br[pl.ds(pl.multiple_of(y * sub, sub), sub)]
        for copy in rs_copies:
            copy.wait_recv()
        r_t = res_ref[...] + ((rs[0] + rs[1]) + (rs[2] + rs[3]) if n_y == 4 else sum(rs[i] for i in range(n_y)))

        st[index] = jnp.concatenate([jnp.sum(r_t, axis=0, keepdims=True), jnp.sum(r_t * r_t, axis=0, keepdims=True),
                                     jnp.zeros((6, rows), jnp.float32)], axis=0)
        st_copies = [start(st.at[index], st.at[index], st_sem, (j,), dy=dy, dchip=dchip, dcore=dcore)
                     for j, (dy, dchip, dcore) in enumerate(offsets)]
        for copy in st_copies:
            copy.wait_recv()
        stats = jnp.sum(st[...], axis=0)
        mean = stats[0:1] / width
        var = stats[1:2] / width - mean * mean

        def f_block(s, dy):
            source = lax.rem(chip - s + n_chip, n_chip) * CORES + core
            begin = source * depth + lax.rem(y - dy + n_y, n_y) * sub
            return f_ref.at[pl.ds(pl.multiple_of(begin, sub), sub)]

        own = f_block(0, 0)
        own[...] = ((r_t - mean) * lax.rsqrt(var + EPS) * gain_ref[...]).astype(jnp.bfloat16)
        fx_copies = {s: start(own, own, fx_sem, (s,), dchip=s) for s in far}
        fy_copies, fd_copies = {}, []
        for s in [0] + far:
            block = f_block(s, 0)
            if s:
                fx_copies[s].wait_recv()
            for dy in range(1, n_y):
                fy_copies[s, dy] = start(block, block, fy_sem, (s, dy), dy=dy)
            fd_copies.append(start(block, block, fd_sem, (s, 0), dcore=1))
        for (s, dy), copy in fy_copies.items():
            copy.wait_recv()
            block = f_block(s, dy)
            fd_copies.append(start(block, block, fd_sem, (s, dy), dcore=1))
        for copy in fd_copies:
            copy.wait_recv()
        sent += [*m_copies.values(), *o_copies, *md_copies, *rs_copies, *st_copies, *fx_copies.values(), *fy_copies.values(), *fd_copies]
        for copy in sent:
            copy.wait_send()

    dma = pltpu.SemaphoreType.DMA
    return pl.pallas_call(
        kernel,
        out_shape=jax.ShapeDtypeStruct((width, rows), jnp.bfloat16),
        in_specs=[pl.BlockSpec(memory_space=pltpu.VMEM)] * 6,
        out_specs=pl.BlockSpec(memory_space=pltpu.VMEM),
        scratch_shapes=[pltpu.VMEM((2, half, rows), jnp.float32), pltpu.VMEM((n_x * half, rows), jnp.bfloat16),
                        pltpu.VMEM((n_all * seqs, q_cols), jnp.bfloat16), pltpu.VMEM((depth, rows), jnp.float32),
                        pltpu.VMEM((n_y, sub, rows), jnp.float32), pltpu.VMEM((n_all, 8, rows), jnp.float32),
                        dma((2,)), dma((2, n_chip)), dma((2, n_chip)), dma((2, len(offsets))), dma((2, n_y)),
                        dma((2, len(offsets))), dma((2, n_chip)), dma((2, n_chip, n_y)), dma((2, n_chip, n_y))],
        compiler_params=pltpu.CompilerParams(collective_id=collective_id, has_side_effects=True,
                                             vmem_limit_bytes=40 << 20),
        name="mix_and_norm",
    )(gate_up, attn_blocks, res_sub, gain_sub, w_out_t, w_down_t)


def after(value, *others):
    return lax.optimization_barrier((value,) + others)[0]


def solution(mesh):
    y_size = mesh.shape["yax"]
    x_size = mesh.shape["xax"]
    chips = x_size // CORES
    sizes = {"y": y_size, "X": chips, "c": CORES}
    row_spec = P(("dp", "yax", "xax"))

    def send(value, chip_step, core_step):
        pairs = [(i * CORES + c, (i + chip_step) % chips * CORES + (c + core_step) % CORES)
                 for i in range(chips) for c in range(CORES)]
        return lax.ppermute(value, "xax", pairs)

    def send_y(value, step):
        return lax.ppermute(value, "yax", [(i, (i + step) % y_size) for i in range(y_size)])

    def contract(lhs, rhs, dims):
        return lax.dot_general(lhs, rhs, (dims, ((), ())), preferred_element_type=jnp.float32)

    def local_step(hidden, cache_len, k_cache, v_cache, g_attn, w_query, w_key, w_value,
                   w_gate, w_up, w_out, w_down, g_final, embedding):
        rows = hidden.shape[0]
        depth = hidden.shape[1]
        width = depth * x_size
        own_rows = k_cache.shape[0]
        head_dim = k_cache.shape[2]
        q_cols = w_query.shape[1]
        heads = q_cols // head_dim
        ff = w_gate.shape[1]
        ff_chip = ff // chips
        vocab = embedding.shape[0]
        own_vocab = vocab // x_size
        me = my_coords()
        y_idx, x_idx, chip, core = me["y"], lax.axis_index("xax"), me["X"], me["c"]
        own_start = (y_idx * x_size + x_idx) * own_rows

        hid_t = hidden.T
        res_t = hid_t.astype(jnp.float32)
        stats = jnp.stack([jnp.sum(res_t, axis=0), jnp.sum(res_t * res_t, axis=0)])
        (stats,) = exchange([(stats, ("X", "c"), ())], sizes, 1)
        gu_own = pick_columns(after((w_gate, w_up), stats), chip, chips)
        gu_parts = [part if s == 0 else send(part, s, 0) for s, part in enumerate(gu_own)]
        padded = -(-own_vocab // LANES) * LANES
        whole = vocab // LANES * LANES
        emb_t = embedding.T
        tail = jnp.pad(emb_t[:, whole:], ((0, 0), (0, LANES - (vocab - whole))))
        emb_parts = split_vocab(after(emb_t, gu_own[0]), tail, x_size, padded)
        emb_got = {(0, 0): emb_parts[0]}

        stats = jnp.sum(stats, axis=0)
        mean = stats[0] / width
        var = stats[1] / width - mean * mean
        norm_t = ((res_t - mean[None]) * lax.rsqrt(var + EPS)[None] * g_attn[:, None]).astype(jnp.bfloat16)

        group = chips * CORES * own_rows
        q_part = contract(norm_t, w_query, ((0,), (0,)))
        q_part = q_part.reshape(y_size * chips, CORES, own_rows * q_cols // LANES, LANES)
        kv_part = contract(norm_t, jnp.concatenate([w_key, w_value], axis=1), ((0,), (0,)))
        kv_part = lax.dynamic_slice_in_dim(kv_part, y_idx * group, group, axis=0)
        kv_part = kv_part.reshape(chips, CORES, own_rows, 2 * head_dim)
        q_all, kv_all = exchange([(q_part.transpose(1, 0, 2, 3), ("c",), ("c",)),
                                  (kv_part.transpose(1, 0, 2, 3), ("c",), ("c",))], sizes, 2)
        sub = depth // y_size
        norm_sub = lax.dynamic_slice_in_dim(norm_t, y_idx * sub, sub, axis=0)
        q_all, kv_all, norm_sub = exchange(
            [(after(jnp.sum(q_all, axis=0), emb_parts), ("y", "X"), ("y", "X")), (jnp.sum(kv_all, axis=0), ("X",), ("X",)),
             (norm_sub, ("X",), ())], sizes, 3)

        norm_got = jnp.stack([norm_sub] + [send_y(norm_sub, s) for s in range(1, y_size)])

        len_own = lax.dynamic_slice_in_dim(cache_len, own_start, own_rows, axis=0)
        angles = rope_angle(len_own, head_dim)
        query = jnp.sum(q_all.reshape(y_size, chips, own_rows, q_cols), axis=1).astype(jnp.bfloat16)
        query = query.reshape(y_size, own_rows, heads, head_dim).transpose(1, 0, 2, 3)
        query = query.reshape(own_rows, y_size * heads, head_dim)
        query_own = rotary(query.astype(jnp.float32), angles[:, None, :]).astype(jnp.bfloat16)
        kv_own = jnp.sum(kv_all, axis=0).astype(jnp.bfloat16)
        key_own = rotary(kv_own[:, :head_dim].astype(jnp.float32), angles).astype(jnp.bfloat16)
        value_own = kv_own[:, head_dim:]

        def fetch(steps, *gates):
            for step in steps:
                part = emb_parts[step[0] * CORES + step[1]]
                emb_got[step] = send(after(part, *gates) if gates else part, *step)

        fetch([(0, 1), (1, 0), (chips - 1, 0), (1, 1), (chips - 1, 1)], q_all)

        attn_own = attend_local(query_own, k_cache, v_cache, key_own, value_own, len_own)
        attn_blocks = attn_own.reshape(own_rows, y_size, q_cols).transpose(1, 0, 2)

        norm_got = jnp.stack([lax.dynamic_index_in_dim(norm_got, lax.rem(y_idx - i + y_size, y_size), 0, keepdims=False)
                              for i in range(y_size)])
        norm_got = norm_got.transpose(1, 0, 2, 3).reshape(chips, depth, rows)
        gate_up = 0.0
        for s in range(chips):
            block = lax.dynamic_index_in_dim(norm_got, lax.rem(chip - s + chips, chips), 0, keepdims=False)
            gate_up = gate_up + lax.dot_general(gu_parts[s], block, (((1,), (0,)), ((), ())),
                                                preferred_element_type=jnp.float32)
        half = ff_chip // CORES
        gate_up = gate_up.reshape(2, CORES, half, rows).transpose(1, 0, 2, 3)
        attn_blocks = jnp.pad(attn_blocks, ((0, 0), (0, -own_rows % 16), (0, 0)))
        res_sub = lax.dynamic_slice_in_dim(res_t, y_idx * sub, sub, axis=0)
        gain_sub = lax.dynamic_slice_in_dim(g_final, y_idx * sub, sub, axis=0)[:, None]
        f_t = mix_and_norm(gate_up, attn_blocks, res_sub, gain_sub, w_out.T, w_down.T, sizes, width, 4)
        fetch([(2, 0), (2, 1)], f_t)
        f_t = f_t.reshape(x_size, depth, rows)

        logits = 0.0
        for chip_step, core_step in emb_got:
            source = lax.rem(chip - chip_step + chips, chips) * CORES + lax.rem(core + core_step, CORES)
            block = lax.dynamic_index_in_dim(f_t, source, 0, keepdims=False)
            logits = logits + contract(emb_got[chip_step, core_step], block, ((0,), (0,)))
        logits = logits[:own_vocab]
        row_max = jnp.max(logits, axis=0)
        sum_exp = jnp.sum(jnp.exp(logits - row_max[None]), axis=0)
        (shares,) = exchange([(jnp.stack([row_max, sum_exp]), ("y", "X", "c"), ())], sizes, 12)
        top = jnp.max(shares[:, 0], axis=0)
        log_norm = top + jnp.log(jnp.sum(shares[:, 1] * jnp.exp(shares[:, 0] - top[None]), axis=0))
        return key_own, value_own, (logits - log_norm[None]).T, log_norm

    in_specs = (P("dp", "xax"), P("dp"), row_spec, row_spec, P("xax"), P("xax", "yax"),
                P("xax", None), P("xax", None), P("xax", "yax"), P("xax", "yax"),
                P("yax", "xax"), P("yax", "xax"), P("xax"), P("yax", "xax"))
    out_specs = (row_spec, row_spec, P("dp", ("yax", "xax")), P("dp"))
    return jax.shard_map(local_step, mesh=mesh, in_specs=in_specs, out_specs=out_specs, check_vma=False)
```
